8 devices in a mesh: dp: 1 (over z), cp: 8 (over y, x, core).
Axes of the slice: x: 2, y: 2, z: 1, core: 2. Of those that a mesh axis runs over, the one named last changes fastest.
Arguments:
- hidden: bfloat16 [8192, 2048], P(('dp', 'cp'))
- seg_id: int32 [8192], P(('dp', 'cp'))
- doc_pos: int32 [8192], P(('dp', 'cp'))
- norm_gain: bfloat16 [2048], replicated
- w_qkv: bfloat16 [2048, 2560], replicated
- b_qkv: bfloat16 [2560], replicated
- w_out: bfloat16 [2048, 2048], replicated
- grad_out: bfloat16 [8192, 2048], P(('dp', 'cp'))
Outputs:
- output 1: bfloat16 [8192, 2048], P(('dp', 'cp'))
- output 2: bfloat16 [8192, 2048], P(('dp', 'cp'))
- output 3: float32 [2048], P('dp')
- output 4: float32 [2048, 2560], P('dp')
- output 5: float32 [2560], P('dp')
- output 6: float32 [2048, 2048], P('dp')
All inputs are finite; a program needn't handle non-finite values.
Results may differ from the reference program's by a relative error of at most 0.0188089.
Values are sent between devices in bfloat16 or wider.
A program may use at most 1 GiB of HBM per device.

```python
import jax
import jax.numpy as jnp
from jax import lax

D = 2048
HEADS = 16
GROUPS = 2
HEAD = 128
SEQ = 8192
DOCS = 4
BLOCK = 128

ROT_DIMS = HEAD // 2
REP_HEADS = HEADS // GROUPS
ATT_WIDTH = HEADS * HEAD
KV_WIDTH = GROUPS * HEAD
QKV_WIDTH = ATT_WIDTH + 2 * KV_WIDTH
ROPE_BASE = 5000000.0
EPS_NORM = 1e-5
NEG_BIG = -1e30


def draw_documents(doc_key):
    cut_points = jax.random.permutation(doc_key, SEQ - 1)[: DOCS - 1] + 1
    start_flag = jnp.zeros((SEQ,), jnp.int32).at[cut_points].set(1)
    seg_id = jnp.cumsum(start_flag).astype(jnp.int32)
    tok_index = jnp.arange(SEQ, dtype=jnp.int32)
    doc_start = lax.cummax(jnp.where(start_flag > 0, tok_index, 0), axis=0)
    return seg_id, (tok_index - doc_start).astype(jnp.int32)


def setup_inputs(seed: int = 0, part: int = 0) -> dict:
    root_key = jax.random.key(seed)
    key_gain, key_wqkv, key_bqkv, key_wout = jax.random.split(root_key, 4)
    part_key = jax.random.fold_in(root_key, part)
    key_x, key_doc, key_dy = jax.random.split(part_key, 3)
    seg_id, doc_pos = draw_documents(key_doc)
    hidden = jax.random.normal(key_x, (SEQ, D), jnp.float32)
    norm_gain = 1.0 + 0.3 * jax.random.normal(key_gain, (D,), jnp.float32)
    w_qkv = 1.5 * D ** -0.5 * jax.random.normal(key_wqkv, (D, QKV_WIDTH), jnp.float32)
    b_qkv = 0.5 * jax.random.normal(key_bqkv, (QKV_WIDTH,), jnp.float32)
    w_out = ATT_WIDTH ** -0.5 * jax.random.normal(key_wout, (ATT_WIDTH, D), jnp.float32)
    grad_out = jax.random.normal(key_dy, (SEQ, D), jnp.float32)
    return {
        'hidden': hidden.astype(jnp.bfloat16),
        'seg_id': seg_id,
        'doc_pos': doc_pos,
        'norm_gain': norm_gain.astype(jnp.bfloat16),
        'w_qkv': w_qkv.astype(jnp.bfloat16),
        'b_qkv': b_qkv.astype(jnp.bfloat16),
        'w_out': w_out.astype(jnp.bfloat16),
        'grad_out': grad_out.astype(jnp.bfloat16),
    }


def rotate(values, cos_ang, sin_ang):
    rot_pairs = values[..., :ROT_DIMS].reshape(values.shape[:-1] + (ROT_DIMS // 2, 2))
    even_part = rot_pairs[..., 0]
    odd_part = rot_pairs[..., 1]
    turned = jnp.stack([even_part * cos_ang - odd_part * sin_ang, odd_part * cos_ang + even_part * sin_ang], axis=-1)
    return jnp.concatenate([turned.reshape(values.shape[:-1] + (ROT_DIMS,)), values[..., ROT_DIMS:]], axis=-1)


def attention_core(q_rot, k_rot, v_val, seg_id):
    n_blocks = SEQ // BLOCK
    scale = HEAD ** -0.5
    q_blocks = q_rot.reshape(n_blocks, BLOCK, GROUPS, REP_HEADS, HEAD)
    k_blocks = k_rot.reshape(n_blocks, BLOCK, GROUPS, HEAD)
    v_blocks = v_val.reshape(n_blocks, BLOCK, GROUPS, HEAD)
    seg_blocks = seg_id.reshape(n_blocks, BLOCK)
    offsets = jnp.arange(BLOCK)

    def query_block(blk_args):
        q_idx, q_blk, seg_q = blk_args

        def key_step(loop_vals, key_args):
            k_idx, k_blk, v_blk, seg_k = key_args
            vis_mask = (seg_q[:, None] == seg_k[None, :]) & (k_idx * BLOCK + offsets[None, :] <= q_idx * BLOCK + offsets[:, None])

            def advance(run_state):
                m_run, l_run, acc_sum = run_state
                scores = jnp.einsum('qgrd,kgd->grqk', q_blk, k_blk) * scale
                scores = jnp.where(vis_mask, scores, NEG_BIG)
                m_new = jnp.maximum(m_run, jnp.max(scores, axis=-1))
                p_mat = jnp.where(vis_mask, jnp.exp(scores - m_new[..., None]), 0.0)
                rescale = jnp.exp(m_run - m_new)
                return (m_new, l_run * rescale + jnp.sum(p_mat, axis=-1), acc_sum * rescale[..., None] + jnp.einsum('grqk,kgd->grqd', p_mat, v_blk))

            return lax.cond(jnp.any(vis_mask), advance, lambda run_state: run_state, loop_vals), None

        init_state = (
            jnp.full((GROUPS, REP_HEADS, BLOCK), NEG_BIG, jnp.float32),
            jnp.zeros((GROUPS, REP_HEADS, BLOCK), jnp.float32),
            jnp.zeros((GROUPS, REP_HEADS, BLOCK, HEAD), jnp.float32),
        )
        final_state, _ = lax.scan(jax.checkpoint(key_step), init_state, (jnp.arange(n_blocks), k_blocks, v_blocks, seg_blocks))
        return final_state[2] / final_state[1][..., None]

    context = lax.map(jax.checkpoint(query_block), (jnp.arange(n_blocks), q_blocks, seg_blocks))
    return context.transpose(0, 3, 1, 2, 4).reshape(SEQ, GROUPS, REP_HEADS, HEAD)


def reference(hidden, seg_id, doc_pos, norm_gain, w_qkv, b_qkv, w_out, grad_out):
    hid_f32 = hidden.astype(jnp.float32)
    inv_rms = lax.rsqrt(jnp.mean(hid_f32 * hid_f32, axis=-1, keepdims=True) + EPS_NORM)
    x_hat = hid_f32 * inv_rms
    gain_f32 = norm_gain.astype(jnp.float32)
    normed = (x_hat * gain_f32).astype(jnp.bfloat16)
    qkv_out = (jnp.dot(normed, w_qkv, preferred_element_type=jnp.float32) + b_qkv.astype(jnp.float32)).astype(jnp.bfloat16)
    inv_freq = ROPE_BASE ** (-jnp.arange(0, ROT_DIMS, 2).astype(jnp.float32) / ROT_DIMS)
    angles = doc_pos.astype(jnp.float32)[:, None] * inv_freq[None, :]
    cos_q = jnp.cos(angles)[:, None, None, :]
    sin_q = jnp.sin(angles)[:, None, None, :]
    cos_k = jnp.cos(angles)[:, None, :]
    sin_k = jnp.sin(angles)[:, None, :]
    q_rot = rotate(qkv_out[:, :ATT_WIDTH].astype(jnp.float32).reshape(SEQ, GROUPS, REP_HEADS, HEAD), cos_q, sin_q).astype(jnp.bfloat16)
    k_rot = rotate(qkv_out[:, ATT_WIDTH:ATT_WIDTH + KV_WIDTH].astype(jnp.float32).reshape(SEQ, GROUPS, HEAD), cos_k, sin_k).astype(jnp.bfloat16)
    v_val = qkv_out[:, ATT_WIDTH + KV_WIDTH:].reshape(SEQ, GROUPS, HEAD)
    ctx_f32, attn_vjp = jax.vjp(
        lambda q_in, k_in, v_in: attention_core(q_in, k_in, v_in, seg_id),
        q_rot.astype(jnp.float32), k_rot.astype(jnp.float32), v_val.astype(jnp.float32))
    context = ctx_f32.astype(jnp.bfloat16).reshape(SEQ, ATT_WIDTH)
    y_out = (hid_f32 + jnp.dot(context, w_out, preferred_element_type=jnp.float32)).astype(jnp.bfloat16)
    grad_ctx = jnp.dot(grad_out, w_out.T, preferred_element_type=jnp.float32).astype(jnp.bfloat16)
    grad_wout = jnp.dot(context.T, grad_out, preferred_element_type=jnp.float32)
    d_query, d_key, d_value = attn_vjp(grad_ctx.astype(jnp.float32).reshape(SEQ, GROUPS, REP_HEADS, HEAD))
    grad_qkv = jnp.concatenate([
        rotate(d_query, cos_q, -sin_q).reshape(SEQ, ATT_WIDTH),
        rotate(d_key, cos_k, -sin_k).reshape(SEQ, KV_WIDTH),
        d_value.reshape(SEQ, KV_WIDTH)], axis=1).astype(jnp.bfloat16)
    grad_bqkv = jnp.sum(grad_qkv.astype(jnp.float32), axis=0)
    grad_wqkv = jnp.dot(normed.T, grad_qkv, preferred_element_type=jnp.float32)
    grad_normed = jnp.dot(grad_qkv, w_qkv.T, preferred_element_type=jnp.float32)
    grad_gain = jnp.sum(grad_normed * x_hat, axis=0)
    scaled = grad_normed * gain_f32
    grad_hidden = (grad_out.astype(jnp.float32) + inv_rms * (scaled - x_hat * jnp.mean(scaled * x_hat, axis=-1, keepdims=True))).astype(jnp.bfloat16)
    return (y_out, grad_hidden, grad_gain, grad_wqkv, grad_bqkv, grad_wout)
```

```python
import functools

import jax
import jax.numpy as jnp
import numpy as np
from jax import lax
from jax.experimental import pallas as pl
from jax.experimental.pallas import tpu as pltpu
from jax.sharding import PartitionSpec as P

HEAD_DIM = 128
ROT_DIMS = 64
ROPE_BASE = 5000000.0
EPS_NORM = 1e-5
MASKED = -1e30
M_START = -1e29
LOG2E = 1.4426950408889634
F32 = jnp.float32
BF16 = jnp.bfloat16

BLK_Q = 256
BLK_K = 512
HEADS = 4
PART = HEADS * HEAD_DIM

NT = (((1,), (1,)), ((), ()))
NN = (((1,), (0,)), ((), ()))
TN = (((0,), (0,)), ((), ()))


def mm(lhs, rhs, dims=NN):
    return lax.dot_general(lhs, rhs, dims, preferred_element_type=F32)


def resident(shape, index_map):
    return pl.BlockSpec(shape, index_map, pipeline_mode=pl.Buffered(1))


def cost(flops, nbytes):
    return pl.CostEstimate(flops=flops, bytes_accessed=nbytes, transcendentals=0)


def head_cols(hh):
    return slice(hh * HEAD_DIM, (hh + 1) * HEAD_DIM)


def turn(slab, cos_tab, sin_tab):
    lane = lax.broadcasted_iota(jnp.int32, slab.shape, 1)
    swapped = jnp.where(lane % 2 == 0, pltpu.roll(slab, HEAD_DIM - 1, 1), pltpu.roll(slab, 1, 1))
    return slab * cos_tab + swapped * sin_tab


def norm_kv_kernel(groups, hid_ref, gain_ref, w_ref, b_ref, cos_ref, sin_ref, normed_ref, kv_ref):
    hid = hid_ref[...].astype(F32)
    inv_rms = lax.rsqrt(jnp.mean(hid * hid, axis=-1, keepdims=True) + EPS_NORM)
    normed = (hid * inv_rms * gain_ref[...].astype(F32)).astype(BF16)
    normed_ref[...] = normed
    out = (mm(normed, w_ref[...]) + b_ref[...].astype(F32)).astype(BF16)
    for gg in range(groups):
        kv_ref[:, head_cols(gg)] = turn(out[:, head_cols(gg)].astype(F32), cos_ref[...], sin_ref[...]).astype(BF16)
        kv_ref[:, head_cols(groups + gg)] = out[:, head_cols(groups + gg)]


def norm_kv(hidden, gain, w_qkv, b_qkv, cos_tab, sin_tab, att_width, tile=256):
    rows, width = hidden.shape
    cols = w_qkv.shape[1] - att_width
    skip = att_width // cols
    return pl.pallas_call(
        functools.partial(norm_kv_kernel, cols // HEAD_DIM // 2),
        grid=(rows // tile,),
        in_specs=[
            pl.BlockSpec((tile, width), lambda i: (i, 0)),
            pl.BlockSpec((1, width), lambda i: (0, 0)),
            pl.BlockSpec((width, cols), lambda i: (0, skip)),
            pl.BlockSpec((1, cols), lambda i: (0, skip)),
            pl.BlockSpec((tile, HEAD_DIM), lambda i: (i, 0)),
            pl.BlockSpec((tile, HEAD_DIM), lambda i: (i, 0)),
        ],
        out_specs=[pl.BlockSpec((tile, width), lambda i: (i, 0)), pl.BlockSpec((tile, cols), lambda i: (i, 0))],
        out_shape=[jax.ShapeDtypeStruct((rows, width), BF16), jax.ShapeDtypeStruct((rows, cols), BF16)],
        cost_estimate=cost(2 * rows * width * cols, 4 * rows * width),
        name='norm_kv',
    )(hidden, gain, w_qkv, b_qkv, cos_tab, sin_tab)


def project_kernel(tab_ref, x_ref, w_ref, b_ref, cos_ref, sin_ref, q_ref):
    out = (mm(x_ref[...], w_ref[...]) + b_ref[...].astype(F32)).astype(BF16)
    for hh in range(HEADS):
        q_ref[:, head_cols(hh)] = turn(out[:, head_cols(hh)].astype(F32), cos_ref[...], sin_ref[...]).astype(BF16)


def project(tab, x, w_qkv, b_qkv, cos_tab, sin_tab, tile=512):
    rows, width = x.shape
    grid_spec = pltpu.PrefetchScalarGridSpec(
        num_scalar_prefetch=1,
        grid=(2, rows // tile),
        in_specs=[
            pl.BlockSpec((tile, width), lambda j, i, t: (i, 0)),
            pl.BlockSpec((width, PART), lambda j, i, t: (0, 2 * t[3, 0] + j)),
            pl.BlockSpec((1, PART), lambda j, i, t: (0, 2 * t[3, 0] + j)),
            pl.BlockSpec((tile, HEAD_DIM), lambda j, i, t: (i, 0)),
            pl.BlockSpec((tile, HEAD_DIM), lambda j, i, t: (i, 0)),
        ],
        out_specs=pl.BlockSpec((tile, PART), lambda j, i, t: (i, j)),
    )
    return pl.pallas_call(
        project_kernel, grid_spec=grid_spec,
        out_shape=jax.ShapeDtypeStruct((rows, 2 * PART), BF16),
        cost_estimate=cost(4 * rows * width * PART, 4 * rows * width),
        name='project',
    )(tab, x, w_qkv, b_qkv, cos_tab, sin_tab)


def block_ranges(tab_ref, qb):
    q_start = tab_ref[0, qb]
    first_doc = tab_ref[1, qb]
    last_doc = tab_ref[2, qb]
    lo = first_doc // BLK_K
    hi = (q_start + BLK_Q - 1) // BLK_K + 1
    full_lo = jnp.clip((last_doc + BLK_K - 1) // BLK_K, lo, hi)
    full_hi = jnp.clip((q_start + 1) // BLK_K, full_lo, hi)
    return q_start, lo, full_lo, full_hi, hi


def visit_blocks(visit, lo, full_lo, full_hi, hi):
    before = full_lo - lo

    def masked_step(idx, _):
        visit(jnp.where(idx < before, lo + idx, full_hi + idx - before), True)
        return 0

    def full_step(kb, _):
        visit(kb, False)
        return 0

    lax.fori_loop(full_lo, full_hi, full_step, 0)
    lax.fori_loop(0, before + (hi - full_hi), masked_step, 0)


def visible(kb, q_start, start_row):
    key_pos = kb * BLK_K + lax.broadcasted_iota(jnp.int32, (BLK_K, BLK_Q), 0)
    q_pos = q_start + lax.broadcasted_iota(jnp.int32, (BLK_K, BLK_Q), 1)
    return (key_pos <= q_pos) & (key_pos >= start_row)


def forward_kernel(tab_ref, q_ref, k_ref, v_ref, start_ref, gctx_ref, ctx_ref, stat_ref, acc_ref, m_ref, l_ref):
    scale2 = HEAD_DIM ** -0.5 * LOG2E
    heads = range(HEADS)
    q_start, lo, full_lo, full_hi, hi = block_ranges(tab_ref, pl.program_id(0))
    acc_ref[...] = jnp.zeros_like(acc_ref)
    m_ref[...] = jnp.full_like(m_ref, M_START)
    l_ref[...] = jnp.zeros_like(l_ref)

    def visit(kb, use_mask):
        rows = pl.ds(pl.multiple_of(kb * BLK_K, BLK_K), BLK_K)
        k_blk = k_ref[rows, :]
        v_turn = v_ref[rows, :].T
        scores = [mm(k_blk, q_ref[:, head_cols(hh)], NT) for hh in heads]
        if use_mask:
            vis = visible(kb, q_start, start_ref[0])
            scores = [jnp.where(vis, sc, MASKED) for sc in scores]
        m_old = [m_ref[hh:hh + 1, :] for hh in heads]
        m_new = [jnp.maximum(m_old[hh], jnp.max(scores[hh], axis=0, keepdims=True)) for hh in heads]
        alpha = [jnp.exp2((m_old[hh] - m_new[hh]) * scale2) for hh in heads]
        p_mat = [jnp.exp2(scores[hh] * scale2 - m_new[hh] * scale2) for hh in heads]
        l_new = [l_ref[hh:hh + 1, :] * alpha[hh] + jnp.sum(p_mat[hh], axis=0, keepdims=True) for hh in heads]
        acc = [acc_ref[hh] * alpha[hh] + mm(v_turn, p_mat[hh].astype(BF16)) for hh in heads]
        for hh in heads:
            m_ref[hh:hh + 1, :] = m_new[hh]
            l_ref[hh:hh + 1, :] = l_new[hh]
            acc_ref[hh] = acc[hh]

    visit_blocks(visit, lo, full_lo, full_hi, hi)

    for hh in heads:
        l_run = l_ref[hh:hh + 1, :]
        ctx_turn = acc_ref[hh] / l_run
        ctx_ref[:, head_cols(hh)] = ctx_turn.T.astype(BF16)
        gctx_turn = gctx_ref[:, head_cols(hh)].astype(F32).T
        stat_ref[0, hh:hh + 1, :] = m_ref[hh:hh + 1, :] * scale2 + jnp.log2(l_run)
        stat_ref[0, HEADS + hh:HEADS + hh + 1, :] = jnp.sum(ctx_turn * gctx_turn, axis=0, keepdims=True)


def forward_attention(part, tab, q, kv_all, start_rows, gctx):
    rows = q.shape[0]
    n_qb = rows // BLK_Q
    n_keys = kv_all.shape[0]
    grid_spec = pltpu.PrefetchScalarGridSpec(
        num_scalar_prefetch=1,
        grid=(n_qb,),
        in_specs=[
            pl.BlockSpec((BLK_Q, PART), lambda i, t: (i, part)),
            resident((n_keys, HEAD_DIM), lambda i, t: (0, t[3, 0])),
            resident((n_keys, HEAD_DIM), lambda i, t: (0, 2 + t[3, 0])),
            pl.BlockSpec((1, 1, BLK_Q), lambda i, t: (i, 0, 0)),
            pl.BlockSpec((BLK_Q, PART), lambda i, t: (i, part)),
        ],
        out_specs=[
            pl.BlockSpec((BLK_Q, PART), lambda i, t: (i, 0)),
            pl.BlockSpec((1, 2 * HEADS, BLK_Q), lambda i, t: (i, 0, 0)),
        ],
        scratch_shapes=[
            pltpu.VMEM((HEADS, HEAD_DIM, BLK_Q), F32),
            pltpu.VMEM((HEADS, BLK_Q), F32),
            pltpu.VMEM((HEADS, BLK_Q), F32),
        ],
    )
    return pl.pallas_call(
        forward_kernel, grid_spec=grid_spec,
        out_shape=[
            jax.ShapeDtypeStruct((rows, PART), BF16),
            jax.ShapeDtypeStruct((n_qb, 2 * HEADS, BLK_Q), F32),
        ],
        cost_estimate=cost(30 * 10 ** 9, 10 * 10 ** 6),
        name='forward_attention',
    )(tab, q, kv_all, kv_all, start_rows, gctx)


def backward_kernel(has_init, tab_ref, q_ref, k_ref, v_ref, start_ref, gctx_ref, stat_ref, cos_ref, sin_ref, *rest):
    init_ref = rest[0] if has_init else None
    dq_ref, dkv_ref, acc_ref = rest[-3:]
    scale = HEAD_DIM ** -0.5
    scale2 = scale * LOG2E
    heads = range(HEADS)
    qb = pl.program_id(0)
    q_start, lo, full_lo, full_hi, hi = block_ranges(tab_ref, qb)

    @pl.when(qb == 0)
    def _():
        dkv_ref[...] = init_ref[...] if has_init else jnp.zeros_like(dkv_ref)

    acc_ref[...] = jnp.zeros_like(acc_ref)

    def visit(kb, use_mask):
        rows = pl.ds(pl.multiple_of(kb * BLK_K, BLK_K), BLK_K)
        k_blk = k_ref[rows, :]
        v_blk = v_ref[rows, :]
        k_turn = k_blk.T
        q_hd = [q_ref[:, head_cols(hh)] for hh in heads]
        g_hd = [gctx_ref[:, head_cols(hh)] for hh in heads]
        scores = [mm(k_blk, q_hd[hh], NT) for hh in heads]
        d_prob = [mm(v_blk, g_hd[hh], NT) for hh in heads]
        p_mat = [jnp.exp2(scores[hh] * scale2 - stat_ref[0, hh:hh + 1, :]) for hh in heads]
        if use_mask:
            vis = visible(kb, q_start, start_ref[0])
            p_mat = [jnp.where(vis, pm, 0.0) for pm in p_mat]
        d_score = [(p_mat[hh] * (d_prob[hh] - stat_ref[0, HEADS + hh:HEADS + hh + 1, :])).astype(BF16) for hh in heads]
        p_low = [pm.astype(BF16) for pm in p_mat]
        d_val = mm(jnp.concatenate(p_low, axis=1), jnp.concatenate(g_hd, axis=0))
        d_key = mm(jnp.concatenate(d_score, axis=1), jnp.concatenate(q_hd, axis=0))
        d_query = [acc_ref[hh] + mm(k_turn, d_score[hh]) for hh in heads]
        for hh in heads:
            acc_ref[hh] = d_query[hh]
        dkv_ref[rows, :HEAD_DIM] += d_key * scale
        dkv_ref[rows, HEAD_DIM:] += d_val

    visit_blocks(visit, lo, full_lo, full_hi, hi)

    cos_tab = cos_ref[...]
    sin_tab = -sin_ref[...]
    for hh in heads:
        dq_ref[:, head_cols(hh)] = turn(acc_ref[hh].T * scale, cos_tab, sin_tab).astype(BF16)


def backward_attention(part, tab, q, kv_all, start_rows, gctx, stats, cos_tab, sin_tab, init):
    rows = q.shape[0]
    n_qb = rows // BLK_Q
    n_keys = kv_all.shape[0]
    grid_spec = pltpu.PrefetchScalarGridSpec(
        num_scalar_prefetch=1,
        grid=(n_qb,),
        in_specs=[
            pl.BlockSpec((BLK_Q, PART), lambda i, t: (i, part)),
            resident((n_keys, HEAD_DIM), lambda i, t: (0, t[3, 0])),
            resident((n_keys, HEAD_DIM), lambda i, t: (0, 2 + t[3, 0])),
            pl.BlockSpec((1, 1, BLK_Q), lambda i, t: (i, 0, 0)),
            pl.BlockSpec((BLK_Q, PART), lambda i, t: (i, part)),
            pl.BlockSpec((1, 2 * HEADS, BLK_Q), lambda i, t: (i, 0, 0)),
            pl.BlockSpec((BLK_Q, HEAD_DIM), lambda i, t: (i, 0)),
            pl.BlockSpec((BLK_Q, HEAD_DIM), lambda i, t: (i, 0)),
        ] + ([] if init is None else [resident((n_keys, 2 * HEAD_DIM), lambda i, t: (0, 0))]),
        out_specs=[
            pl.BlockSpec((BLK_Q, PART), lambda i, t: (i, 0)),
            resident((n_keys, 2 * HEAD_DIM), lambda i, t: (0, 0)),
        ],
        scratch_shapes=[pltpu.VMEM((HEADS, HEAD_DIM, BLK_Q), F32)],
    )
    return pl.pallas_call(
        functools.partial(backward_kernel, init is not None), grid_spec=grid_spec,
        out_shape=[
            jax.ShapeDtypeStruct((rows, PART), BF16),
            jax.ShapeDtypeStruct((n_keys, 2 * HEAD_DIM), F32),
        ],
        cost_estimate=cost(75 * 10 ** 9, 20 * 10 ** 6),
        name='backward_attention',
    )(tab, q, kv_all, kv_all, start_rows, gctx, stats, cos_tab, sin_tab, *([] if init is None else [init]))


def finish_kv_kernel(tab_ref, d_ref, cos_ref, sin_ref, out_ref):
    out_ref[:, :HEAD_DIM] = turn(d_ref[:, :HEAD_DIM], cos_ref[...], -sin_ref[...]).astype(BF16)
    out_ref[:, HEAD_DIM:] = d_ref[:, HEAD_DIM:].astype(BF16)


def finish_kv(tab, d_kv, cos_tab, sin_tab):
    rows, cols = d_kv.shape
    tile = rows // 2
    grid_spec = pltpu.PrefetchScalarGridSpec(
        num_scalar_prefetch=1,
        grid=(2,),
        in_specs=[
            pl.BlockSpec((tile, cols), lambda i, t: (i ^ t[3, 0], 0)),
            pl.BlockSpec((tile, HEAD_DIM), lambda i, t: (i, 0)),
            pl.BlockSpec((tile, HEAD_DIM), lambda i, t: (i, 0)),
        ],
        out_specs=pl.BlockSpec((tile, cols), lambda i, t: (i, 0)),
    )
    return pl.pallas_call(
        finish_kv_kernel, grid_spec=grid_spec,
        out_shape=jax.ShapeDtypeStruct((rows, cols), BF16),
        cost_estimate=cost(10 ** 6, 6 * rows * cols),
        name='finish_kv',
    )(tab, d_kv, cos_tab, sin_tab)


def place_q_kernel(tab_ref, a_mine, a_far, b_mine, b_far, out_ref):
    for core in range(2):
        @pl.when(tab_ref[3, 0] == core)
        def _(core=core):
            for idx, ref in enumerate((a_mine, b_mine)):
                out_ref[:, (2 * core + idx) * PART:(2 * core + idx + 1) * PART] = ref[...]
            for idx, ref in enumerate((a_far, b_far)):
                out_ref[:, (2 * (1 - core) + idx) * PART:(2 * (1 - core) + idx + 1) * PART] = ref[...]


def place_q(tab, pieces, cols, tile=256):
    rows = pieces[0].shape[0]
    grid_spec = pltpu.PrefetchScalarGridSpec(
        num_scalar_prefetch=1,
        grid=(rows // tile,),
        in_specs=[pl.BlockSpec((tile, PART), lambda i, t: (i, 0))] * 4,
        out_specs=pl.BlockSpec((tile, 4 * PART), lambda i, t: (i, 0)),
    )
    return pl.pallas_call(
        place_q_kernel, grid_spec=grid_spec,
        out_shape=jax.ShapeDtypeStruct((rows, cols), F32),
        cost_estimate=cost(10 ** 6, 8 * rows * cols),
        name='place_q',
    )(tab, *pieces)


def place_kv_kernel(tab_ref, mine, far, whole_ref, out_ref):
    for core in range(2):
        @pl.when(tab_ref[3, 0] == core)
        def _(core=core):
            for idx in range(2):
                out_ref[:, head_cols(2 * idx + core)] = mine[:, head_cols(idx)]
                out_ref[:, head_cols(2 * idx + 1 - core)] = far[:, head_cols(idx)]


def place_kv(tab, mine, far, whole, tile=512):
    rows, cols = whole.shape
    width = 4 * HEAD_DIM
    last = cols // width - 1
    grid_spec = pltpu.PrefetchScalarGridSpec(
        num_scalar_prefetch=1,
        grid=(rows // tile,),
        in_specs=[pl.BlockSpec((tile, 2 * HEAD_DIM), lambda i, t: (i, 0))] * 2 + [pl.BlockSpec(memory_space=pl.ANY)],
        out_specs=pl.BlockSpec((tile, width), lambda i, t: (i, last)),
    )
    return pl.pallas_call(
        place_kv_kernel, grid_spec=grid_spec,
        out_shape=jax.ShapeDtypeStruct((rows, cols), F32),
        input_output_aliases={3: 0},
        cost_estimate=cost(10 ** 6, 8 * rows * width),
        name='place_kv',
    )(tab, mine, far, whole)


def solution(mesh):
    n_ctx = mesh.shape['cp']
    swap = [(dev, dev ^ 1) for dev in range(n_ctx)]
    chips = [[dev for dev in range(n_ctx) if dev % 2 == core] for core in range(2)]
    lanes = np.arange(HEAD_DIM)
    freq = np.where(lanes < ROT_DIMS, ROPE_BASE ** (-(lanes // 2 * 2).astype(np.float64) / ROT_DIMS), 0.0).astype(np.float32)
    sign = np.where(lanes % 2 == 0, -1.0, 1.0).astype(np.float32)

    def per_device(hidden, seg_id, doc_pos, norm_gain, w_qkv, b_qkv, w_out, grad_out):
        n_rows, hid_width = hidden.shape
        att_width = w_out.shape[0]
        half = att_width // 2
        me = lax.axis_index('cp')
        core = me % 2
        other = 1 - core

        def swapped(arr):
            return lax.ppermute(arr, 'cp', swap)

        def chip_sum(arrs):
            return lax.psum(arrs, 'cp', axis_index_groups=chips)

        def after(arr, earlier):
            return lax.optimization_barrier((arr, earlier))[0]

        def tables(pos):
            angles = pos.astype(F32)[:, None] * freq[None, :]
            return jnp.cos(angles), jnp.sin(angles) * sign[None, :]

        pos_far = swapped(doc_pos)
        grad_far = swapped(grad_out)
        cos_own, sin_own = tables(doc_pos)
        gain2 = norm_gain[None, :]
        bias2 = b_qkv[None, :]
        normed, kv_own = norm_kv(hidden, gain2, w_qkv, bias2, cos_own, sin_own, att_width)
        kv_all = lax.all_gather(kv_own, 'cp', axis=0, tiled=True)
        normed_far = swapped(normed)
        cos_far, sin_far = tables(pos_far)
        cos_tab = jnp.concatenate([cos_own, cos_far], axis=0)
        sin_tab = jnp.concatenate([sin_own, sin_far], axis=0)
        normed2 = jnp.concatenate([normed, normed_far], axis=0)
        grad2 = jnp.concatenate([grad_out, grad_far], axis=0)
        pos2 = jnp.concatenate([doc_pos, pos_far])
        row_ids = jnp.concatenate([me * n_rows + jnp.arange(n_rows), (me + 1 - 2 * core) * n_rows + jnp.arange(n_rows)]).astype(jnp.int32)
        start_rows = row_ids - pos2
        n_qb = 2 * n_rows // BLK_Q
        tab = jnp.stack([row_ids[::BLK_Q], start_rows[::BLK_Q], start_rows[BLK_Q - 1::BLK_Q], jnp.full((n_qb,), core, jnp.int32)])
        start3 = start_rows.reshape(n_qb, 1, BLK_Q)

        q_rot = project(tab, normed2, w_qkv, bias2, cos_tab, sin_tab)
        wo_mine = lax.dynamic_slice_in_dim(w_out, core * half, half, 0)
        wo_far = lax.dynamic_slice_in_dim(w_out, other * half, half, 0)
        gctx = mm(grad2, wo_mine, NT).astype(BF16)

        ctx = []
        stats = []
        grad_wo = []
        for part in range(2):
            ctx_part, stat_part = forward_attention(part, tab, q_rot, kv_all, start3, gctx)
            ctx.append(ctx_part)
            stats.append(stat_part)
            grad_wo.append(mm(ctx_part, grad2, TN))

        grad_wo = list(chip_sum(tuple(grad_wo)))

        hid_f32 = hidden.astype(F32)
        y_sum = hid_f32
        for part in range(2):
            rows = slice(part * PART, (part + 1) * PART)
            y_sum = y_sum + mm(ctx[part][:n_rows], wo_mine[rows]) + mm(swapped(ctx[part][n_rows:]), wo_far[rows])
        y_out = y_sum.astype(BF16)

        d_query = []
        grad_q = []
        d_kv = None
        for part in range(2):
            dq_part, d_kv = backward_attention(part, tab, q_rot, kv_all, start3, gctx, stats[part], cos_tab, sin_tab, d_kv)
            d_query.append(dq_part)
            grad_q.append(mm(normed2, dq_part, TN))

        grad_q[0] = chip_sum(after(grad_q[0], grad_wo))
        d_kv = lax.psum_scatter(after(d_kv, grad_q[0]), 'cp', scatter_dimension=0, tiled=True, axis_index_groups=chips)
        d_kv = finish_kv(tab, d_kv, cos_tab, sin_tab)
        grad_q[1], grad_kv = chip_sum((after(grad_q[1], d_kv), mm(normed2, d_kv, TN)))

        def w_cols(first, count):
            return lax.dynamic_slice_in_dim(w_qkv, first, count, 1)

        grad_normed = (mm(d_kv[:n_rows, :HEAD_DIM], w_cols(att_width + core * HEAD_DIM, HEAD_DIM), NT)
                       + mm(d_kv[:n_rows, HEAD_DIM:], w_cols(att_width + (2 + core) * HEAD_DIM, HEAD_DIM), NT))
        dkv_far = swapped(d_kv[n_rows:])
        grad_normed += (mm(dkv_far[:, :HEAD_DIM], w_cols(att_width + other * HEAD_DIM, HEAD_DIM), NT)
                        + mm(dkv_far[:, HEAD_DIM:], w_cols(att_width + (2 + other) * HEAD_DIM, HEAD_DIM), NT))
        for part in range(2):
            grad_normed += mm(d_query[part][:n_rows], w_cols(core * half + part * PART, PART), NT)
            grad_normed += mm(swapped(d_query[part][n_rows:]), w_cols(other * half + part * PART, PART), NT)
        inv_rms = lax.rsqrt(jnp.mean(hid_f32 * hid_f32, axis=-1, keepdims=True) + EPS_NORM)
        x_hat = hid_f32 * inv_rms
        gain_f32 = norm_gain.astype(F32)
        scaled = grad_normed * gain_f32
        grad_hidden = (grad_out.astype(F32) + inv_rms * (scaled - x_hat * jnp.mean(scaled * x_hat, axis=-1, keepdims=True))).astype(BF16)

        def col_sum(arr):
            return jnp.sum(arr.astype(F32), axis=0)

        bias_q = jnp.concatenate([col_sum(dq) for dq in d_query])
        bias_kv = col_sum(d_kv)
        none_q = jnp.zeros_like(bias_q)
        none_kv = jnp.zeros((HEAD_DIM,), F32)
        low = core == 0

        def two(vec, zero):
            return [jnp.where(low, vec, zero), jnp.where(low, zero, vec)]

        small = jnp.concatenate(two(bias_q, none_q) + two(bias_kv[:HEAD_DIM], none_kv) + two(bias_kv[HEAD_DIM:], none_kv)
                                + [jnp.sum(grad_normed * x_hat, axis=0)])
        for step in (1, 2, 4):
            small = small + lax.ppermute(small, 'cp', [(dev, dev ^ step) for dev in range(n_ctx)])
        grad_bqkv = small[:w_qkv.shape[1]]
        grad_gain = small[w_qkv.shape[1]:]

        wo_pieces = grad_wo + [swapped(arr) for arr in grad_wo]
        grad_wout = jnp.concatenate([jnp.where(low, wo_pieces[idx], wo_pieces[idx ^ 2]) for idx in range(4)], axis=0)
        whole = place_q(tab, (grad_q[0], swapped(grad_q[0]), grad_q[1], swapped(grad_q[1])), w_qkv.shape[1])
        grad_wqkv = place_kv(tab, grad_kv, swapped(grad_kv), whole)
        return y_out, grad_hidden, grad_gain, grad_wqkv, grad_bqkv, grad_wout

    act_spec = P(('dp', 'cp'), None)
    row_spec = P(('dp', 'cp'))
    return jax.shard_map(per_device, mesh=mesh,
                         in_specs=(act_spec, row_spec, row_spec, P(), P(), P(), P(), act_spec),
                         out_specs=(act_spec, act_spec, P('dp'), P('dp', None), P('dp'), P('dp', None)),
                         check_vma=False)
```

```python
import functools

import jax
import jax.numpy as jnp
import numpy as np
from jax import lax
from jax.experimental import pallas as pl
from jax.experimental.pallas import tpu as pltpu
from jax.sharding import PartitionSpec as P

HEAD_DIM = 128
ROT_DIMS = 64
ROPE_BASE = 5000000.0
EPS_NORM = 1e-5
MASKED = -1e30
M_START = -1e29
LOG2E = 1.4426950408889634
F32 = jnp.float32
BF16 = jnp.bfloat16

BLK_Q = 256
BLK_K = 512
HEADS = 4
PART = HEADS * HEAD_DIM

NT = (((1,), (1,)), ((), ()))
NN = (((1,), (0,)), ((), ()))
TN = (((0,), (0,)), ((), ()))


def mm(lhs, rhs, dims=NN):
    return lax.dot_general(lhs, rhs, dims, preferred_element_type=F32)


def resident(shape, index_map):
    return pl.BlockSpec(shape, index_map, pipeline_mode=pl.Buffered(1))


def cost(flops, nbytes):
    return pl.CostEstimate(flops=flops, bytes_accessed=nbytes, transcendentals=0)


def head_cols(hh):
    return slice(hh * HEAD_DIM, (hh + 1) * HEAD_DIM)


def turn(slab, cos_tab, sin_tab):
    lane = lax.broadcasted_iota(jnp.int32, slab.shape, 1)
    swapped = jnp.where(lane % 2 == 0, pltpu.roll(slab, HEAD_DIM - 1, 1), pltpu.roll(slab, 1, 1))
    return slab * cos_tab + swapped * sin_tab


def norm_kv_kernel(groups, hid_ref, gain_ref, w_ref, b_ref, cos_ref, sin_ref, normed_ref, kv_ref):
    hid = hid_ref[...].astype(F32)
    inv_rms = lax.rsqrt(jnp.mean(hid * hid, axis=-1, keepdims=True) + EPS_NORM)
    normed = (hid * inv_rms * gain_ref[...].astype(F32)).astype(BF16)
    normed_ref[...] = normed
    out = (mm(normed, w_ref[...]) + b_ref[...].astype(F32)).astype(BF16)
    for gg in range(groups):
        kv_ref[:, head_cols(gg)] = turn(out[:, head_cols(gg)].astype(F32), cos_ref[...], sin_ref[...]).astype(BF16)
        kv_ref[:, head_cols(groups + gg)] = out[:, head_cols(groups + gg)]


def norm_kv(hidden, gain, w_qkv, b_qkv, cos_tab, sin_tab, att_width, tile=256):
    rows, width = hidden.shape
    cols = w_qkv.shape[1] - att_width
    skip = att_width // cols
    return pl.pallas_call(
        functools.partial(norm_kv_kernel, cols // HEAD_DIM // 2),
        grid=(rows // tile,),
        in_specs=[
            pl.BlockSpec((tile, width), lambda i: (i, 0)),
            pl.BlockSpec((1, width), lambda i: (0, 0)),
            pl.BlockSpec((width, cols), lambda i: (0, skip)),
            pl.BlockSpec((1, cols), lambda i: (0, skip)),
            pl.BlockSpec((tile, HEAD_DIM), lambda i: (i, 0)),
            pl.BlockSpec((tile, HEAD_DIM), lambda i: (i, 0)),
        ],
        out_specs=[pl.BlockSpec((tile, width), lambda i: (i, 0)), pl.BlockSpec((tile, cols), lambda i: (i, 0))],
        out_shape=[jax.ShapeDtypeStruct((rows, width), BF16), jax.ShapeDtypeStruct((rows, cols), BF16)],
        cost_estimate=cost(2 * rows * width * cols, 4 * rows * width),
        name='norm_kv',
    )(hidden, gain, w_qkv, b_qkv, cos_tab, sin_tab)


def project_kernel(tab_ref, x_ref, w_ref, b_ref, cos_ref, sin_ref, q_ref):
    out = (mm(x_ref[...], w_ref[...]) + b_ref[...].astype(F32)).astype(BF16)
    for hh in range(HEADS):
        q_ref[:, head_cols(hh)] = turn(out[:, head_cols(hh)].astype(F32), cos_ref[...], sin_ref[...]).astype(BF16)


def project(tab, x, w_qkv, b_qkv, cos_tab, sin_tab, tile=512):
    rows, width = x.shape
    grid_spec = pltpu.PrefetchScalarGridSpec(
        num_scalar_prefetch=1,
        grid=(2, rows // tile),
        in_specs=[
            pl.BlockSpec((tile, width), lambda j, i, t: (i, 0)),
            pl.BlockSpec((width, PART), lambda j, i, t: (0, 2 * t[3, 0] + j)),
            pl.BlockSpec((1, PART), lambda j, i, t: (0, 2 * t[3, 0] + j)),
            pl.BlockSpec((tile, HEAD_DIM), lambda j, i, t: (i, 0)),
            pl.BlockSpec((tile, HEAD_DIM), lambda j, i, t: (i, 0)),
        ],
        out_specs=pl.BlockSpec((tile, PART), lambda j, i, t: (i, j)),
    )
    return pl.pallas_call(
        project_kernel, grid_spec=grid_spec,
        out_shape=jax.ShapeDtypeStruct((rows, 2 * PART), BF16),
        cost_estimate=cost(4 * rows * width * PART, 4 * rows * width),
        name='project',
    )(tab, x, w_qkv, b_qkv, cos_tab, sin_tab)


def block_ranges(tab_ref, qb):
    q_start = tab_ref[0, qb]
    first_doc = tab_ref[1, qb]
    last_doc = tab_ref[2, qb]
    lo = first_doc // BLK_K
    hi = (q_start + BLK_Q - 1) // BLK_K + 1
    full_lo = jnp.clip((last_doc + BLK_K - 1) // BLK_K, lo, hi)
    full_hi = jnp.clip((q_start + 1) // BLK_K, full_lo, hi)
    return q_start, lo, full_lo, full_hi, hi


def visit_blocks(visit, lo, full_lo, full_hi, hi):
    before = full_lo - lo

    def masked_step(idx, _):
        visit(jnp.where(idx < before, lo + idx, full_hi + idx - before), True)
        return 0

    def full_step(kb, _):
        visit(kb, False)
        return 0

    lax.fori_loop(full_lo, full_hi, full_step, 0)
    lax.fori_loop(0, before + (hi - full_hi), masked_step, 0)


def visible(kb, q_start, start_row):
    key_pos = kb * BLK_K + lax.broadcasted_iota(jnp.int32, (BLK_K, BLK_Q), 0)
    q_pos = q_start + lax.broadcasted_iota(jnp.int32, (BLK_K, BLK_Q), 1)
    return (key_pos <= q_pos) & (key_pos >= start_row)


def forward_kernel(tab_ref, q_ref, k_ref, v_ref, start_ref, gctx_ref, ctx_ref, stat_ref, acc_ref, m_ref, l_ref):
    scale2 = HEAD_DIM ** -0.5 * LOG2E
    heads = range(HEADS)
    q_start, lo, full_lo, full_hi, hi = block_ranges(tab_ref, pl.program_id(0))
    acc_ref[...] = jnp.zeros_like(acc_ref)
    m_ref[...] = jnp.full_like(m_ref, M_START)
    l_ref[...] = jnp.zeros_like(l_ref)

    def visit(kb, use_mask):
        rows = pl.ds(pl.multiple_of(kb * BLK_K, BLK_K), BLK_K)
        k_blk = k_ref[rows, :]
        v_turn = v_ref[rows, :].T
        scores = [mm(k_blk, q_ref[:, head_cols(hh)], NT) for hh in heads]
        if use_mask:
            vis = visible(kb, q_start, start_ref[0])
            scores = [jnp.where(vis, sc, MASKED) for sc in scores]
        m_old = [m_ref[hh:hh + 1, :] for hh in heads]
        m_new = [jnp.maximum(m_old[hh], jnp.max(scores[hh], axis=0, keepdims=True)) for hh in heads]
        alpha = [jnp.exp2((m_old[hh] - m_new[hh]) * scale2) for hh in heads]
        p_mat = [jnp.exp2(scores[hh] * scale2 - m_new[hh] * scale2) for hh in heads]
        l_new = [l_ref[hh:hh + 1, :] * alpha[hh] + jnp.sum(p_mat[hh], axis=0, keepdims=True) for hh in heads]
        acc = [acc_ref[hh] * alpha[hh] + mm(v_turn, p_mat[hh].astype(BF16)) for hh in heads]
        for hh in heads:
            m_ref[hh:hh + 1, :] = m_new[hh]
            l_ref[hh:hh + 1, :] = l_new[hh]
            acc_ref[hh] = acc[hh]

    visit_blocks(visit, lo, full_lo, full_hi, hi)

    for hh in heads:
        l_run = l_ref[hh:hh + 1, :]
        ctx_turn = acc_ref[hh] / l_run
        ctx_ref[:, head_cols(hh)] = ctx_turn.T.astype(BF16)
        gctx_turn = gctx_ref[:, head_cols(hh)].astype(F32).T
        stat_ref[0, hh:hh + 1, :] = m_ref[hh:hh + 1, :] * scale2 + jnp.log2(l_run)
        stat_ref[0, HEADS + hh:HEADS + hh + 1, :] = jnp.sum(ctx_turn * gctx_turn, axis=0, keepdims=True)


def forward_attention(part, tab, q, kv_all, start_rows, gctx):
    rows = q.shape[0]
    n_qb = rows // BLK_Q
    n_keys = kv_all.shape[0]
    grid_spec = pltpu.PrefetchScalarGridSpec(
        num_scalar_prefetch=1,
        grid=(n_qb,),
        in_specs=[
            pl.BlockSpec((BLK_Q, PART), lambda i, t: (i, part)),
            resident((n_keys, HEAD_DIM), lambda i, t: (0, t[3, 0])),
            resident((n_keys, HEAD_DIM), lambda i, t: (0, 2 + t[3, 0])),
            pl.BlockSpec((1, 1, BLK_Q), lambda i, t: (i, 0, 0)),
            pl.BlockSpec((BLK_Q, PART), lambda i, t: (i, part)),
        ],
        out_specs=[
            pl.BlockSpec((BLK_Q, PART), lambda i, t: (i, 0)),
            pl.BlockSpec((1, 2 * HEADS, BLK_Q), lambda i, t: (i, 0, 0)),
        ],
        scratch_shapes=[
            pltpu.VMEM((HEADS, HEAD_DIM, BLK_Q), F32),
            pltpu.VMEM((HEADS, BLK_Q), F32),
            pltpu.VMEM((HEADS, BLK_Q), F32),
        ],
    )
    return pl.pallas_call(
        forward_kernel, grid_spec=grid_spec,
        out_shape=[
            jax.ShapeDtypeStruct((rows, PART), BF16),
            jax.ShapeDtypeStruct((n_qb, 2 * HEADS, BLK_Q), F32),
        ],
        cost_estimate=cost(30 * 10 ** 9, 10 * 10 ** 6),
        name='forward_attention',
    )(tab, q, kv_all, kv_all, start_rows, gctx)


def backward_kernel(has_init, tab_ref, q_ref, k_ref, v_ref, start_ref, gctx_ref, stat_ref, cos_ref, sin_ref, *rest):
    init_ref = rest[0] if has_init else None
    dq_ref, dkv_ref, acc_ref = rest[-3:]
    scale = HEAD_DIM ** -0.5
    scale2 = scale * LOG2E
    heads = range(HEADS)
    qb = pl.program_id(0)
    q_start, lo, full_lo, full_hi, hi = block_ranges(tab_ref, qb)

    @pl.when(qb == 0)
    def _():
        dkv_ref[...] = init_ref[...] if has_init else jnp.zeros_like(dkv_ref)

    acc_ref[...] = jnp.zeros_like(acc_ref)

    def visit(kb, use_mask):
        rows = pl.ds(pl.multiple_of(kb * BLK_K, BLK_K), BLK_K)
        k_blk = k_ref[rows, :]
        v_blk = v_ref[rows, :]
        k_turn = k_blk.T
        q_hd = [q_ref[:, head_cols(hh)] for hh in heads]
        g_hd = [gctx_ref[:, head_cols(hh)] for hh in heads]
        scores = [mm(k_blk, q_hd[hh], NT) for hh in heads]
        d_prob = [mm(v_blk, g_hd[hh], NT) for hh in heads]
        p_mat = [jnp.exp2(scores[hh] * scale2 - stat_ref[0, hh:hh + 1, :]) for hh in heads]
        if use_mask:
            vis = visible(kb, q_start, start_ref[0])
            p_mat = [jnp.where(vis, pm, 0.0) for pm in p_mat]
        d_score = [(p_mat[hh] * (d_prob[hh] - stat_ref[0, HEADS + hh:HEADS + hh + 1, :])).astype(BF16) for hh in heads]
        p_low = [pm.astype(BF16) for pm in p_mat]
        d_val = mm(jnp.concatenate(p_low, axis=1), jnp.concatenate(g_hd, axis=0))
        d_key = mm(jnp.concatenate(d_score, axis=1), jnp.concatenate(q_hd, axis=0))
        d_query = [acc_ref[hh] + mm(k_turn, d_score[hh]) for hh in heads]
        for hh in heads:
            acc_ref[hh] = d_query[hh]
        dkv_ref[rows, :HEAD_DIM] += d_key * scale
        dkv_ref[rows, HEAD_DIM:] += d_val

    visit_blocks(visit, lo, full_lo, full_hi, hi)

    cos_tab = cos_ref[...]
    sin_tab = -sin_ref[...]
    for hh in heads:
        dq_ref[:, head_cols(hh)] = turn(acc_ref[hh].T * scale, cos_tab, sin_tab).astype(BF16)


def backward_attention(part, tab, q, kv_all, start_rows, gctx, stats, cos_tab, sin_tab, init):
    rows = q.shape[0]
    n_qb = rows // BLK_Q
    n_keys = kv_all.shape[0]
    grid_spec = pltpu.PrefetchScalarGridSpec(
        num_scalar_prefetch=1,
        grid=(n_qb,),
        in_specs=[
            pl.BlockSpec((BLK_Q, PART), lambda i, t: (i, part)),
            resident((n_keys, HEAD_DIM), lambda i, t: (0, t[3, 0])),
            resident((n_keys, HEAD_DIM), lambda i, t: (0, 2 + t[3, 0])),
            pl.BlockSpec((1, 1, BLK_Q), lambda i, t: (i, 0, 0)),
            pl.BlockSpec((BLK_Q, PART), lambda i, t: (i, part)),
            pl.BlockSpec((1, 2 * HEADS, BLK_Q), lambda i, t: (i, 0, 0)),
            pl.BlockSpec((BLK_Q, HEAD_DIM), lambda i, t: (i, 0)),
            pl.BlockSpec((BLK_Q, HEAD_DIM), lambda i, t: (i, 0)),
        ] + ([] if init is None else [resident((n_keys, 2 * HEAD_DIM), lambda i, t: (0, 0))]),
        out_specs=[
            pl.BlockSpec((BLK_Q, PART), lambda i, t: (i, 0)),
            resident((n_keys, 2 * HEAD_DIM), lambda i, t: (0, 0)),
        ],
        scratch_shapes=[pltpu.VMEM((HEADS, HEAD_DIM, BLK_Q), F32)],
    )
    return pl.pallas_call(
        functools.partial(backward_kernel, init is not None), grid_spec=grid_spec,
        out_shape=[
            jax.ShapeDtypeStruct((rows, PART), BF16),
            jax.ShapeDtypeStruct((n_keys, 2 * HEAD_DIM), F32),
        ],
        cost_estimate=cost(75 * 10 ** 9, 20 * 10 ** 6),
        name='backward_attention',
    )(tab, q, kv_all, kv_all, start_rows, gctx, stats, cos_tab, sin_tab, *([] if init is None else [init]))


def finish_kv_kernel(tab_ref, d_ref, cos_ref, sin_ref, out_ref):
    out_ref[:, :HEAD_DIM] = turn(d_ref[:, :HEAD_DIM], cos_ref[...], -sin_ref[...]).astype(BF16)
    out_ref[:, HEAD_DIM:] = d_ref[:, HEAD_DIM:].astype(BF16)


def finish_kv(tab, d_kv, cos_tab, sin_tab):
    rows, cols = d_kv.shape
    tile = rows // 2
    grid_spec = pltpu.PrefetchScalarGridSpec(
        num_scalar_prefetch=1,
        grid=(2,),
        in_specs=[
            pl.BlockSpec((tile, cols), lambda i, t: (i ^ t[3, 0], 0)),
            pl.BlockSpec((tile, HEAD_DIM), lambda i, t: (i, 0)),
            pl.BlockSpec((tile, HEAD_DIM), lambda i, t: (i, 0)),
        ],
        out_specs=pl.BlockSpec((tile, cols), lambda i, t: (i, 0)),
    )
    return pl.pallas_call(
        finish_kv_kernel, grid_spec=grid_spec,
        out_shape=jax.ShapeDtypeStruct((rows, cols), BF16),
        cost_estimate=cost(10 ** 6, 6 * rows * cols),
        name='finish_kv',
    )(tab, d_kv, cos_tab, sin_tab)


def place_q_kernel(tab_ref, a_mine, a_far, b_mine, b_far, out_ref):
    for core in range(2):
        @pl.when(tab_ref[3, 0] == core)
        def _(core=core):
            for idx, ref in enumerate((a_mine, b_mine)):
                out_ref[:, (2 * core + idx) * PART:(2 * core + idx + 1) * PART] = ref[...]
            for idx, ref in enumerate((a_far, b_far)):
                out_ref[:, (2 * (1 - core) + idx) * PART:(2 * (1 - core) + idx + 1) * PART] = ref[...]


def place_q(tab, pieces, cols, tile=256):
    rows = pieces[0].shape[0]
    grid_spec = pltpu.PrefetchScalarGridSpec(
        num_scalar_prefetch=1,
        grid=(rows // tile,),
        in_specs=[pl.BlockSpec((tile, PART), lambda i, t: (i, 0))] * 4,
        out_specs=pl.BlockSpec((tile, 4 * PART), lambda i, t: (i, 0)),
    )
    return pl.pallas_call(
        place_q_kernel, grid_spec=grid_spec,
        out_shape=jax.ShapeDtypeStruct((rows, cols), F32),
        cost_estimate=cost(10 ** 6, 8 * rows * cols),
        name='place_q',
    )(tab, *pieces)


def place_kv_kernel(tab_ref, mine, far, whole_ref, out_ref):
    for core in range(2):
        @pl.when(tab_ref[3, 0] == core)
        def _(core=core):
            for idx in range(2):
                out_ref[:, head_cols(2 * idx + core)] = mine[:, head_cols(idx)]
                out_ref[:, head_cols(2 * idx + 1 - core)] = far[:, head_cols(idx)]


def place_kv(tab, mine, far, whole, tile=512):
    rows, cols = whole.shape
    width = 4 * HEAD_DIM
    last = cols // width - 1
    grid_spec = pltpu.PrefetchScalarGridSpec(
        num_scalar_prefetch=1,
        grid=(rows // tile,),
        in_specs=[pl.BlockSpec((tile, 2 * HEAD_DIM), lambda i, t: (i, 0))] * 2 + [pl.BlockSpec(memory_space=pl.ANY)],
        out_specs=pl.BlockSpec((tile, width), lambda i, t: (i, last)),
    )
    return pl.pallas_call(
        place_kv_kernel, grid_spec=grid_spec,
        out_shape=jax.ShapeDtypeStruct((rows, cols), F32),
        input_output_aliases={3: 0},
        cost_estimate=cost(10 ** 6, 8 * rows * width),
        name='place_kv',
    )(tab, mine, far, whole)


def solution(mesh):
    n_ctx = mesh.shape['cp']
    swap = [(dev, dev ^ 1) for dev in range(n_ctx)]
    chips = [[dev for dev in range(n_ctx) if dev % 2 == core] for core in range(2)]
    lanes = np.arange(HEAD_DIM)
    freq = np.where(lanes < ROT_DIMS, ROPE_BASE ** (-(lanes // 2 * 2).astype(np.float64) / ROT_DIMS), 0.0).astype(np.float32)
    sign = np.where(lanes % 2 == 0, -1.0, 1.0).astype(np.float32)

    def per_device(hidden, seg_id, doc_pos, norm_gain, w_qkv, b_qkv, w_out, grad_out):
        n_rows, hid_width = hidden.shape
        att_width = w_out.shape[0]
        half = att_width // 2
        me = lax.axis_index('cp')
        core = me % 2
        other = 1 - core

        def swapped(arr):
            return lax.ppermute(arr, 'cp', swap)

        def chip_sum(arrs):
            return lax.psum(arrs, 'cp', axis_index_groups=chips)

        def after(arr, earlier):
            return lax.optimization_barrier((arr, earlier))[0]

        def tables(pos):
            angles = pos.astype(F32)[:, None] * freq[None, :]
            return jnp.cos(angles), jnp.sin(angles) * sign[None, :]

        pos_far = swapped(doc_pos)
        grad_far = swapped(grad_out)
        cos_own, sin_own = tables(doc_pos)
        gain2 = norm_gain[None, :]
        bias2 = b_qkv[None, :]
        normed, kv_own = norm_kv(hidden, gain2, w_qkv, bias2, cos_own, sin_own, att_width)
        kv_all = lax.all_gather(kv_own, 'cp', axis=0, tiled=True)
        normed_far = swapped(normed)
        cos_far, sin_far = tables(pos_far)
        cos_tab = jnp.concatenate([cos_own, cos_far], axis=0)
        sin_tab = jnp.concatenate([sin_own, sin_far], axis=0)
        normed2 = jnp.concatenate([normed, normed_far], axis=0)
        grad2 = jnp.concatenate([grad_out, grad_far], axis=0)
        pos2 = jnp.concatenate([doc_pos, pos_far])
        row_ids = jnp.concatenate([me * n_rows + jnp.arange(n_rows), (me + 1 - 2 * core) * n_rows + jnp.arange(n_rows)]).astype(jnp.int32)
        start_rows = row_ids - pos2
        n_qb = 2 * n_rows // BLK_Q
        tab = jnp.stack([row_ids[::BLK_Q], start_rows[::BLK_Q], start_rows[BLK_Q - 1::BLK_Q], jnp.full((n_qb,), core, jnp.int32)])
        start3 = start_rows.reshape(n_qb, 1, BLK_Q)

        q_rot = project(tab, normed2, w_qkv, bias2, cos_tab, sin_tab)
        wo_mine = lax.dynamic_slice_in_dim(w_out, core * half, half, 0)
        wo_far = lax.dynamic_slice_in_dim(w_out, other * half, half, 0)
        gctx = mm(grad2, wo_mine, NT).astype(BF16)

        ctx = []
        stats = []
        grad_wo = []
        for part in range(2):
            ctx_part, stat_part = forward_attention(part, tab, q_rot, kv_all, start3, gctx)
            ctx.append(ctx_part)
            stats.append(stat_part)
            wo_part = mm(ctx_part, grad2, TN)
            grad_wo.append(chip_sum(wo_part if part == 0 else after(wo_part, grad_wo[0])))

        hid_f32 = hidden.astype(F32)
        y_sum = hid_f32
        for part in range(2):
            rows = slice(part * PART, (part + 1) * PART)
            y_sum = y_sum + mm(ctx[part][:n_rows], wo_mine[rows]) + mm(swapped(ctx[part][n_rows:]), wo_far[rows])
        y_out = y_sum.astype(BF16)

        d_query = []
        grad_q = []
        d_kv = None
        for part in range(2):
            dq_part, d_kv = backward_attention(part, tab, q_rot, kv_all, start3, gctx, stats[part], cos_tab, sin_tab, d_kv)
            d_query.append(dq_part)
            grad_q.append(mm(normed2, dq_part, TN))

        grad_q[0] = chip_sum(after(grad_q[0], grad_wo))
        d_kv = lax.psum_scatter(after(d_kv, grad_q[0]), 'cp', scatter_dimension=0, tiled=True, axis_index_groups=chips)
        d_kv = finish_kv(tab, d_kv, cos_tab, sin_tab)
        grad_q[1], grad_kv = chip_sum((after(grad_q[1], d_kv), mm(normed2, d_kv, TN)))

        def w_cols(first, count):
            return lax.dynamic_slice_in_dim(w_qkv, first, count, 1)

        grad_normed = (mm(d_kv[:n_rows, :HEAD_DIM], w_cols(att_width + core * HEAD_DIM, HEAD_DIM), NT)
                       + mm(d_kv[:n_rows, HEAD_DIM:], w_cols(att_width + (2 + core) * HEAD_DIM, HEAD_DIM), NT))
        dkv_far = swapped(d_kv[n_rows:])
        grad_normed += (mm(dkv_far[:, :HEAD_DIM], w_cols(att_width + other * HEAD_DIM, HEAD_DIM), NT)
                        + mm(dkv_far[:, HEAD_DIM:], w_cols(att_width + (2 + other) * HEAD_DIM, HEAD_DIM), NT))
        for part in range(2):
            grad_normed += mm(d_query[part][:n_rows], w_cols(core * half + part * PART, PART), NT)
            grad_normed += mm(swapped(d_query[part][n_rows:]), w_cols(other * half + part * PART, PART), NT)
        inv_rms = lax.rsqrt(jnp.mean(hid_f32 * hid_f32, axis=-1, keepdims=True) + EPS_NORM)
        x_hat = hid_f32 * inv_rms
        gain_f32 = norm_gain.astype(F32)
        scaled = grad_normed * gain_f32
        grad_hidden = (grad_out.astype(F32) + inv_rms * (scaled - x_hat * jnp.mean(scaled * x_hat, axis=-1, keepdims=True))).astype(BF16)

        def col_sum(arr):
            return jnp.sum(arr.astype(F32), axis=0)

        bias_q = jnp.concatenate([col_sum(dq) for dq in d_query])
        bias_kv = col_sum(d_kv)
        none_q = jnp.zeros_like(bias_q)
        none_kv = jnp.zeros((HEAD_DIM,), F32)
        low = core == 0

        def two(vec, zero):
            return [jnp.where(low, vec, zero), jnp.where(low, zero, vec)]

        small = jnp.concatenate(two(bias_q, none_q) + two(bias_kv[:HEAD_DIM], none_kv) + two(bias_kv[HEAD_DIM:], none_kv)
                                + [jnp.sum(grad_normed * x_hat, axis=0)])
        for step in (1, 2, 4):
            small = small + lax.ppermute(small, 'cp', [(dev, dev ^ step) for dev in range(n_ctx)])
        grad_bqkv = small[:w_qkv.shape[1]]
        grad_gain = small[w_qkv.shape[1]:]

        wo_pieces = grad_wo + [swapped(arr) for arr in grad_wo]
        grad_wout = jnp.concatenate([jnp.where(low, wo_pieces[idx], wo_pieces[idx ^ 2]) for idx in range(4)], axis=0)
        whole = place_q(tab, (grad_q[0], swapped(grad_q[0]), grad_q[1], swapped(grad_q[1])), w_qkv.shape[1])
        grad_wqkv = place_kv(tab, grad_kv, swapped(grad_kv), whole)
        return y_out, grad_hidden, grad_gain, grad_wqkv, grad_bqkv, grad_wout

    act_spec = P(('dp', 'cp'), None)
    row_spec = P(('dp', 'cp'))
    return jax.shard_map(per_device, mesh=mesh,
                         in_specs=(act_spec, row_spec, row_spec, P(), P(), P(), P(), act_spec),
                         out_specs=(act_spec, act_spec, P('dp'), P('dp', None), P('dp'), P('dp', None)),
                         check_vma=False)
```
